32 devices in a mesh: replica: 16 (over z, y, core), model: 2 (over x).
Axes of the slice: x: 2, y: 2, z: 4, core: 2. Of those that a mesh axis runs over, the one named last changes fastest.
Arguments:
- layer_grads: bfloat16 [16, 2, 4096, 1024], P('replica', None, 'model'), may hold values from -6 to 6
- last_basis: float32 [2, 1024, 32], replicated, may hold values from -6 to 6
- layer_weights: float32 [2, 4096, 1024], P(None, 'model', 'replica'), may hold values from -0.1875 to 0.1875
- momentum: float32 [2, 4096, 1024], P(None, 'model', 'replica'), may hold values from -0.3125 to 0.3125
Outputs:
- new_weights: float32 [2, 4096, 1024], P(None, 'model', 'replica')
- new_basis: float32 [2, 1024, 32], replicated
- new_momentum: float32 [2, 4096, 1024], P(None, 'model', 'replica')
The draws below stay inside these ranges and needn't reach their ends.
All inputs are finite; a program needn't handle non-finite values.
Results may differ from the reference program's by a relative error of at most 0.0029.
Values sent between devices are 32-bit elements; how exact they have to be, the bound alone decides.
A program may use at most 64 MiB of HBM per device.

```python
import jax
import jax.numpy as jnp
from jax import lax

WIDTH = 1024
INNER = 4096
RANK = 32
LAYERS = 2
REPLICAS = 16
N_MODEL = 2


def draw_layer_grads(key, part):
    keys = jax.random.split(key, 5)
    level = jnp.exp(jax.random.uniform(keys[4], (1, LAYERS, N_MODEL, 1, RANK), jnp.float32, -1.3, 1.3))
    left = jax.random.normal(keys[0], (1, LAYERS, N_MODEL, INNER // N_MODEL, RANK), jnp.float32) * level
    left = left.reshape(1, LAYERS, INNER, RANK)
    right = jax.random.normal(keys[1], (1, LAYERS, RANK, WIDTH), jnp.float32)
    strength = jax.random.normal(keys[2], (REPLICAS, LAYERS, 1, RANK), jnp.float32)
    noise = jax.random.normal(keys[3], (REPLICAS, LAYERS, INNER, WIDTH), jnp.float32)
    low = jnp.einsum('alir,lrw->aliw', left * strength, right[0])
    values = low * RANK ** (-0.5) + 0.5 * noise
    return jnp.clip(values, -6.0, 6.0).astype(jnp.bfloat16)


def block_scale(key, dims, shards, least, high):
    level = 1.0
    for dim, blocks in shards:
        draws = jax.random.uniform(jax.random.fold_in(jax.random.fold_in(key, 6), dim), (blocks,), jnp.float32, least / len(shards), high / len(shards))
        level = level * jnp.repeat(jnp.exp(draws), dims[dim] // blocks).reshape((-1,) + (1,) * (len(dims) - 1 - dim))
    return level


def gaussian(key, shape, width, reach, pieces=(), kind=jnp.bfloat16):
    values = width * jax.random.normal(key, shape, jnp.float32)
    if pieces:
        values = values * block_scale(key, shape, pieces, -0.22, 0.18)
    return jnp.clip(values, -reach, reach).astype(kind)


def setup_inputs(seed: int = 0) -> dict:
    seeds = jax.random.split(jax.random.key(seed), 5)
    layer_grads = draw_layer_grads(jax.random.fold_in(seeds[4], 71), 0)
    last_basis = gaussian(seeds[1], (LAYERS, WIDTH, RANK), 1.0, 6.0, (), jnp.float32)
    layer_weights = gaussian(seeds[2], (LAYERS, INNER, WIDTH), WIDTH ** -0.5, 0.1875, ((1, 2), (2, 16)), jnp.float32)
    momentum = gaussian(seeds[3], (LAYERS, INNER, WIDTH), 0.05, 0.3125, ((1, 2), (2, 16)), jnp.float32)
    return dict(layer_grads=layer_grads, last_basis=last_basis, layer_weights=layer_weights, momentum=momentum)


def reference(layer_grads, last_basis, layer_weights, momentum):
    small_basis = last_basis.astype(jnp.bfloat16)
    small_basis = lax.optimization_barrier(small_basis)
    left = jnp.einsum('aliw,lwr->lir', layer_grads.astype(jnp.float32), small_basis.astype(jnp.float32))
    gram = jnp.einsum('lir,lis->lrs', left, left, precision=lax.Precision.HIGHEST)
    gram = gram + 0.001 * lax.optimization_barrier(jnp.mean(jnp.diagonal(gram, axis1=1, axis2=2), axis=1))[:, None, None] * jnp.eye(RANK, dtype=jnp.float32)
    small_left = lax.optimization_barrier(left.astype(jnp.bfloat16))
    right = jnp.einsum('aliw,lir->lwr', layer_grads.astype(jnp.float32), small_left.astype(jnp.float32))
    root = jnp.linalg.cholesky(gram)
    half = lax.linalg.triangular_solve(root, jnp.swapaxes(right, 1, 2), left_side=True, lower=True)
    mixed = lax.linalg.triangular_solve(root, half, left_side=True, lower=True, transpose_a=True)
    change = jnp.einsum('lir,lrw->liw', left, mixed, precision=lax.Precision.HIGHEST) / REPLICAS
    new_momentum = 0.9 * momentum + change
    new_weights = layer_weights - 0.02 * new_momentum
    new_basis = right * lax.rsqrt(lax.optimization_barrier(jnp.mean(right * right, axis=(1, 2), keepdims=True)) + 1e-12)
    return (new_weights, new_basis, new_momentum)
```

```python
import functools

import jax
import jax.numpy as jnp
from jax import lax
from jax.experimental import pallas as pl
from jax.experimental.pallas import tpu as pltpu
from jax.sharding import PartitionSpec as P

LANES = 128
F32 = jnp.float32
BF16 = jnp.bfloat16
NT = (((1,), (1,)), ((), ()))


def split(value):
    high = value.astype(BF16)
    return high, (value - high.astype(F32)).astype(BF16)


def invert(a, rank, first):
    lane = lax.broadcasted_iota(jnp.int32, a.shape, 1)
    sub = lax.broadcasted_iota(jnp.int32, a.shape, 0)
    for p in range(rank):
        at = first + p
        row = a[p : p + 1, :]
        col = a[:, at : at + 1]
        inverse = 1.0 / a[p : p + 1, at : at + 1]
        row = jnp.where(lane[:1] == at, 1.0, row) * inverse
        a = jnp.where(sub == p, row, jnp.where(lane == at, 0.0, a) - col * row)
    return a


def kernel(
    n, m, grads, basis, weights, momentum, out_w, out_b, out_m,
    g, b, w, mom, stack, part, from_core, summed, arrived, left,
    r_part, r_core, r_sum, r_arrived, r_model, right, gram, basis_out,
    load_sem, core_s, core_r, rs_s, rs_r, ag_s, ag_r, fwd_s, fwd_r,
    mod_s, mod_r,
):
    layers, rows, width = g.shape
    rank = b.shape[2]
    pair = layers * rank
    q = n // 2
    half = rows // 2
    blocks = half // LANES
    wc = width // n
    me = lax.axis_index("replica")
    x = lax.axis_index("model")
    c, k = lax.rem(me, 2), me // 2
    o = 1 - c

    def near(d):
        return lax.rem(k + d, q)

    def before(d):
        return lax.rem(k + q - d, q)

    def send(src, dst, s, r, device):
        copy = pltpu.make_async_remote_copy(
            src_ref=src, dst_ref=dst, send_sem=s, recv_sem=r,
            device_id=device, device_id_type=pl.DeviceIdType.MESH,
        )
        copy.start()
        return copy

    partner = {"replica": 2 * k + o}

    def chip(d):
        return {"replica": 2 * near(d) + c}

    def other(d):
        return {"model": lax.rem(x + d, m)}

    def rows_of(h):
        return pl.ds(pl.multiple_of(h * half, half), half)

    load_b = pltpu.make_async_copy(basis, b, load_sem.at[0])
    load_b.start()
    loads = []
    for i, h in enumerate((o, c)):
        for l in range(layers):
            copy = pltpu.make_async_copy(
                grads.at[0, l, rows_of(h)], g.at[l, rows_of(h)],
                load_sem.at[3 + i * layers + l],
            )
            copy.start()
            loads.append(copy)
    load_m = pltpu.make_async_copy(momentum, mom, load_sem.at[1])
    load_w = pltpu.make_async_copy(weights, w, load_sem.at[2])
    load_m.start()
    load_w.start()

    barrier = pltpu.get_barrier_semaphore()
    peers = [partner] + [chip(d) for d in range(1, q)] + [other(d) for d in range(1, m)]
    for device in peers:
        pl.semaphore_signal(
            barrier, inc=1, device_id=device, device_id_type=pl.DeviceIdType.MESH
        )

    load_b.wait()
    turned = [b[l].T.astype(BF16) for l in range(layers)]

    def part_of(h, i):
        for l in range(layers):
            loads[i * layers + l].wait()
            value = lax.dot_general(
                turned[l], g[l, rows_of(h), :], NT, preferred_element_type=F32
            )
            for j in range(blocks):
                at = pl.multiple_of((h * blocks + j) * pair + l * rank, rank)
                part[pl.ds(at, rank), :] = value[:, j * LANES : (j + 1) * LANES]

    waits = []

    def reduce_scatter(source, near_buf, sums, far_buf, phase, mid, mid2):
        size = source.shape[0] // 2
        share = size // q
        mine = pl.ds(pl.multiple_of(c * size, size), size)
        theirs = pl.ds(pl.multiple_of(o * size, size), size)
        core = send(source.at[theirs], near_buf, core_s.at[phase], core_r.at[phase], partner)
        mid()
        core.wait_recv()
        sums[...] = source[mine, :] + near_buf[...]
        copies = []
        for d in range(1, q):
            to = pl.ds(pl.multiple_of(near(d) * share, share), share)
            copies.append(
                send(sums.at[to], far_buf.at[d - 1], rs_s.at[phase, d - 1],
                     rs_r.at[phase, d - 1], chip(d))
            )
        mid2()
        total = sums[pl.ds(pl.multiple_of(k * share, share), share), :]
        for d in range(1, q):
            copies[d - 1].wait_recv()
            total = total + far_buf[d - 1]
        waits.extend([core] + copies)
        return total

    def gather_start(buf, phase):
        share = buf.shape[0] // n
        own = pl.ds(pl.multiple_of((c * q + k) * share, share), share)
        copies = [
            send(buf.at[own], buf.at[own], ag_s.at[phase, d - 1], ag_r.at[phase, d - 1], chip(d))
            for d in range(1, q)
        ]
        forwards = [
            send(buf.at[own], buf.at[own], fwd_s.at[phase, 0], fwd_r.at[phase, 0], partner)
        ]
        return copies, forwards

    def gather_pass(buf, phase, copies, forwards):
        share = buf.shape[0] // n
        for d in range(1, q):
            copies[d - 1].wait_recv()
            at = pl.ds(pl.multiple_of((c * q + before(d)) * share, share), share)
            forwards.append(
                send(buf.at[at], buf.at[at], fwd_s.at[phase, d], fwd_r.at[phase, d], partner)
            )

    def gather_end(copies, forwards):
        for copy in forwards:
            copy.wait_recv()
        waits.extend(copies + forwards)

    part_of(o, 0)
    pl.semaphore_wait(barrier, len(peers))
    share = reduce_scatter(
        part, from_core, summed, arrived, 0, lambda: part_of(c, 1), lambda: None
    )
    size = part.shape[0] // n
    left[pl.ds(pl.multiple_of((c * q + k) * size, size), size), :] = share
    copies, forwards = gather_start(left, 0)
    gather_pass(left, 0, copies, forwards)

    def lefts(h):
        return [
            jnp.concatenate(
                [
                    left[pl.ds(pl.multiple_of((h * blocks + j) * pair + l * rank, rank), rank), :]
                    for j in range(blocks)
                ],
                axis=1,
            )
            for l in range(layers)
        ]

    def right_of(h):
        return [
            jnp.dot(value.astype(BF16), g[l, rows_of(h), :], preferred_element_type=F32)
            for l, value in enumerate(lefts(h))
        ]

    own_right = right_of(c)
    gather_end(copies, forwards)
    own_right = [a + v for a, v in zip(own_right, right_of(o))]
    if layers * wc < LANES:
        r_part[...] = jnp.zeros_like(r_part)
    for idx in range(n):
        at = ((idx % 2) * q + idx // 2) * rank
        for l in range(layers):
            r_part[at : at + rank, l * wc : (l + 1) * wc] = own_right[l][:, idx * wc : (idx + 1) * wc]

    gram_copies = []

    def make_gram():
        total = jnp.zeros((pair, pair), F32)
        for h in range(2):
            both = jnp.concatenate(lefts(h), axis=0)
            total = total + lax.dot_general(
                both, both, NT, precision=lax.Precision.HIGHEST, preferred_element_type=F32
            )
        gram[x] = jnp.concatenate([total, jnp.zeros((pair, LANES - pair), F32)], axis=1)
        for d in range(1, m):
            gram_copies.append(
                send(gram.at[x], gram.at[x], mod_s.at[0, d - 1], mod_r.at[0, d - 1], other(d))
            )

    inverses = []

    def solve():
        for h in range(2):
            for l, value in enumerate(lefts(h)):
                high, low = split(value)
                stack[l, h * half : (h + 1) * half, :] = jnp.concatenate(
                    [high, high, low, low], axis=0
                ).T
        for copy in gram_copies:
            copy.wait_recv()
        total = gram[0]
        for i in range(1, m):
            total = total + gram[i]
        for l in range(layers):
            a = total[l * rank : (l + 1) * rank, :]
            sub = lax.broadcasted_iota(jnp.int32, a.shape, 0)
            lane = lax.broadcasted_iota(jnp.int32, a.shape, 1)
            diagonal = lane == sub + l * rank
            ridge = 0.001 * jnp.sum(jnp.where(diagonal, a, 0.0)) / rank
            a = a + jnp.where(diagonal, ridge, 0.0)
            a = invert(a, rank, l * rank)
            inside = (lane >= l * rank) & (lane < (l + 1) * rank)
            inverses.append(jnp.where(inside, a, 0.0)[:, :pair])

    total = reduce_scatter(r_part, r_core, r_sum, r_arrived, 1, make_gram, solve)
    waits.extend(gram_copies)
    r_model[x] = total
    swaps = [
        send(r_model.at[x], r_model.at[x], mod_s.at[1, d - 1], mod_r.at[1, d - 1], other(d))
        for d in range(1, m)
    ]
    for copy in swaps:
        copy.wait_recv()
    waits.extend(swaps)
    total = r_model[0]
    for i in range(1, m):
        total = total + r_model[i]
    right[pl.ds(pl.multiple_of((c * q + k) * rank, rank), rank), :] = total
    copies, forwards = gather_start(right, 1)

    mixed = jnp.dot(
        jnp.concatenate(inverses, axis=0),
        jnp.concatenate([total] * layers, axis=0),
        precision=lax.Precision.HIGHEST,
        preferred_element_type=F32,
    ) / n
    load_m.wait()
    load_w.wait()
    stores = []
    for l in range(layers):
        high, low = split(mixed[l * rank : (l + 1) * rank, l * wc : (l + 1) * wc])
        change = jnp.dot(
            stack[l], jnp.concatenate([high, low, high, low], axis=0), preferred_element_type=F32
        )
        new_m = 0.9 * mom[l] + change
        mom[l] = new_m
        w[l] = w[l] - 0.02 * new_m
        for src, dst, i in ((mom, out_m, 0), (w, out_w, 1)):
            copy = pltpu.make_async_copy(src.at[l], dst.at[l], load_sem.at[3 + 2 * l + i])
            copy.start()
            stores.append(copy)

    gather_pass(right, 1, copies, forwards)
    gather_end(copies, forwards)
    squares = jnp.zeros((rank, LANES), F32)
    for pos in range(n):
        value = right[pos * rank : (pos + 1) * rank, :]
        squares = squares + value * value
    lane = lax.broadcasted_iota(jnp.int32, squares.shape, 1)
    scales = [
        lax.rsqrt(
            jnp.sum(
                jnp.where((lane >= l * wc) & (lane < (l + 1) * wc), squares, 0.0),
                axis=(0, 1), keepdims=True,
            ) / (width * rank) + 1e-12
        )
        for l in range(layers)
    ]
    for idx in range(n):
        at = ((idx % 2) * q + idx // 2) * rank
        value = right[at : at + rank, :].T
        for l in range(layers):
            basis_out[l, idx * wc : (idx + 1) * wc, :] = value[l * wc : (l + 1) * wc, :] * scales[l]
    copy = pltpu.make_async_copy(basis_out, out_b, load_sem.at[0])
    copy.start()
    stores.append(copy)
    for copy in waits:
        copy.wait_send()
    for copy in stores:
        copy.wait()


def shards(n, m, layer_grads, last_basis, layer_weights, momentum):
    _, layers, rows, width = layer_grads.shape
    rank = last_basis.shape[2]
    pair = layers * rank
    q = n // 2
    tall = rows // LANES * pair
    dma = pltpu.SemaphoreType.DMA
    vmem = pltpu.VMEM
    return pl.pallas_call(
        functools.partial(kernel, n, m),
        out_shape=(
            jax.ShapeDtypeStruct(layer_weights.shape, F32),
            jax.ShapeDtypeStruct(last_basis.shape, F32),
            jax.ShapeDtypeStruct(momentum.shape, F32),
        ),
        in_specs=[pl.BlockSpec(memory_space=pl.ANY)] * 4,
        out_specs=[pl.BlockSpec(memory_space=pl.ANY)] * 3,
        scratch_shapes=[
            vmem((layers, rows, width), BF16),
            vmem(last_basis.shape, F32),
            vmem(layer_weights.shape, F32),
            vmem(momentum.shape, F32),
            vmem((layers, rows, 4 * rank), BF16),
            vmem((tall, LANES), F32),
            vmem((tall // 2, LANES), F32),
            vmem((tall // 2, LANES), F32),
            vmem((q - 1, tall // n, LANES), F32),
            vmem((tall, LANES), F32),
            vmem((n * rank, LANES), F32),
            vmem((q * rank, LANES), F32),
            vmem((q * rank, LANES), F32),
            vmem((q - 1, rank, LANES), F32),
            vmem((m, rank, LANES), F32),
            vmem((n * rank, LANES), F32),
            vmem((m, pair, LANES), F32),
            vmem(last_basis.shape, F32),
            dma((3 + 2 * layers,)),
            dma((2,)), dma((2,)),
            dma((2, q - 1)), dma((2, q - 1)),
            dma((2, q - 1)), dma((2, q - 1)),
            dma((2, q)), dma((2, q)),
            dma((2, m - 1)), dma((2, m - 1)),
        ],
        compiler_params=pltpu.CompilerParams(
            collective_id=0, has_side_effects=True, vmem_limit_bytes=32 * 1024 * 1024
        ),
        name="step",
    )(layer_grads, last_basis, layer_weights, momentum)


def solution(mesh):
    in_specs = (
        P("replica", None, "model", None),
        P(),
        P(None, "model", "replica"),
        P(None, "model", "replica"),
    )
    out_specs = (P(None, "model", "replica"), P(), P(None, "model", "replica"))
    body = functools.partial(shards, mesh.shape["replica"], mesh.shape["model"])
    return jax.shard_map(body, mesh=mesh, in_specs=in_specs, out_specs=out_specs, check_vma=False)
```

```python
import functools

import jax
import jax.numpy as jnp
from jax import lax
from jax.experimental import pallas as pl
from jax.experimental.pallas import tpu as pltpu
from jax.sharding import PartitionSpec as P

LANES = 128
MIB = 1024 * 1024
LIMIT = 32 * MIB
LIMIT2 = 16 * MIB
F32 = jnp.float32
BF16 = jnp.bfloat16
NT = (((1,), (1,)), ((), ()))


def split(value):
    high = value.astype(BF16)
    return high, (value - high.astype(F32)).astype(BF16)


def invert(a, rank, first):
    lane = lax.broadcasted_iota(jnp.int32, a.shape, 1)
    sub = lax.broadcasted_iota(jnp.int32, a.shape, 0)
    for p in range(rank):
        at = first + p
        row = a[p : p + 1, :]
        col = a[:, at : at + 1]
        inverse = 1.0 / a[p : p + 1, at : at + 1]
        row = jnp.where(lane[:1] == at, 1.0, row) * inverse
        a = jnp.where(sub == p, row, jnp.where(lane == at, 0.0, a) - col * row)
    return a


def kernel(
    n, m, grads, basis, weights, momentum, out_w, out_b, out_m,
    g, b, w, mom, stack, part, from_core, summed, arrived, left,
    r_part, r_core, r_sum, r_arrived, r_model, right, gram, basis_out,
    load_sem, core_s, core_r, rs_s, rs_r, ag_s, ag_r, fwd_s, fwd_r,
    mod_s, mod_r,
):
    layers, rows, width = g.shape
    rank = b.shape[1]
    pair = layers * rank
    q = n // 2
    half = rows // 2
    blocks = half // LANES
    wc = width // n
    me = lax.axis_index("replica")
    x = lax.axis_index("model")
    c, k = lax.rem(me, 2), me // 2
    o = 1 - c

    def near(d):
        return lax.rem(k + d, q)

    def before(d):
        return lax.rem(k + q - d, q)

    def send(src, dst, s, r, device):
        copy = pltpu.make_async_remote_copy(
            src_ref=src, dst_ref=dst, send_sem=s, recv_sem=r,
            device_id=device, device_id_type=pl.DeviceIdType.MESH,
        )
        copy.start()
        return copy

    partner = {"replica": 2 * k + o}

    def chip(d):
        return {"replica": 2 * near(d) + c}

    def other(d):
        return {"model": lax.rem(x + d, m)}

    def rows_of(h):
        return pl.ds(pl.multiple_of(h * half, half), half)

    load_b = pltpu.make_async_copy(basis, b, load_sem.at[0])
    load_b.start()
    loads = []
    for i, h in enumerate((o, c)):
        for l in range(layers):
            copy = pltpu.make_async_copy(
                grads.at[0, l, rows_of(h)], g.at[l, rows_of(h)],
                load_sem.at[3 + i * layers + l],
            )
            copy.start()
            loads.append(copy)
    load_m = pltpu.make_async_copy(momentum, mom, load_sem.at[1])
    load_w = pltpu.make_async_copy(weights, w, load_sem.at[2])
    load_m.start()
    load_w.start()

    barrier = pltpu.get_barrier_semaphore()
    peers = [partner] + [chip(d) for d in range(1, q)] + [other(d) for d in range(1, m)]
    for device in peers:
        pl.semaphore_signal(
            barrier, inc=1, device_id=device, device_id_type=pl.DeviceIdType.MESH
        )

    load_b.wait()
    turned = [b[l].astype(BF16) for l in range(layers)]

    def part_of(h, i):
        for l in range(layers):
            loads[i * layers + l].wait()
            value = lax.dot_general(
                turned[l], g[l, rows_of(h), :], NT, preferred_element_type=F32
            )
            for j in range(blocks):
                at = pl.multiple_of((h * blocks + j) * pair + l * rank, rank)
                part[pl.ds(at, rank), :] = value[:, j * LANES : (j + 1) * LANES]

    waits = []

    def reduce_scatter(source, near_buf, sums, far_buf, phase, mid, mid2):
        size = source.shape[0] // 2
        share = size // q
        mine = pl.ds(pl.multiple_of(c * size, size), size)
        theirs = pl.ds(pl.multiple_of(o * size, size), size)
        core = send(source.at[theirs], near_buf, core_s.at[phase], core_r.at[phase], partner)
        mid()
        core.wait_recv()
        sums[...] = source[mine, :] + near_buf[...]
        copies = []
        for d in range(1, q):
            to = pl.ds(pl.multiple_of(near(d) * share, share), share)
            copies.append(
                send(sums.at[to], far_buf.at[d - 1], rs_s.at[phase, d - 1],
                     rs_r.at[phase, d - 1], chip(d))
            )
        mid2()
        total = sums[pl.ds(pl.multiple_of(k * share, share), share), :]
        for d in range(1, q):
            copies[d - 1].wait_recv()
            total = total + far_buf[d - 1]
        waits.extend([core] + copies)
        return total

    def gather_start(buf, phase):
        share = buf.shape[0] // n
        own = pl.ds(pl.multiple_of((c * q + k) * share, share), share)
        copies = [
            send(buf.at[own], buf.at[own], ag_s.at[phase, d - 1], ag_r.at[phase, d - 1], chip(d))
            for d in range(1, q)
        ]
        forwards = [
            send(buf.at[own], buf.at[own], fwd_s.at[phase, 0], fwd_r.at[phase, 0], partner)
        ]
        return copies, forwards

    def gather_pass(buf, phase, copies, forwards):
        share = buf.shape[0] // n
        for d in range(1, q):
            copies[d - 1].wait_recv()
            at = pl.ds(pl.multiple_of((c * q + before(d)) * share, share), share)
            forwards.append(
                send(buf.at[at], buf.at[at], fwd_s.at[phase, d], fwd_r.at[phase, d], partner)
            )

    def gather_end(copies, forwards):
        for copy in forwards:
            copy.wait_recv()
        waits.extend(copies + forwards)

    part_of(o, 0)
    pl.semaphore_wait(barrier, len(peers))
    share = reduce_scatter(
        part, from_core, summed, arrived, 0, lambda: part_of(c, 1), lambda: None
    )
    size = part.shape[0] // n
    left[pl.ds(pl.multiple_of((c * q + k) * size, size), size), :] = share
    copies, forwards = gather_start(left, 0)
    gather_pass(left, 0, copies, forwards)

    def lefts(h):
        return [
            jnp.concatenate(
                [
                    left[pl.ds(pl.multiple_of((h * blocks + j) * pair + l * rank, rank), rank), :]
                    for j in range(blocks)
                ],
                axis=1,
            )
            for l in range(layers)
        ]

    def right_of(h):
        return [
            jnp.dot(value.astype(BF16), g[l, rows_of(h), :], preferred_element_type=F32)
            for l, value in enumerate(lefts(h))
        ]

    own_right = right_of(c)
    gather_end(copies, forwards)
    own_right = [a + v for a, v in zip(own_right, right_of(o))]
    if layers * wc < LANES:
        r_part[...] = jnp.zeros_like(r_part)
    for idx in range(n):
        at = ((idx % 2) * q + idx // 2) * rank
        for l in range(layers):
            r_part[at : at + rank, l * wc : (l + 1) * wc] = own_right[l][:, idx * wc : (idx + 1) * wc]

    gram_copies = []

    def make_gram():
        total = jnp.zeros((pair, pair), F32)
        for h in range(2):
            both = jnp.concatenate(lefts(h), axis=0)
            total = total + lax.dot_general(
                both, both, NT, precision=lax.Precision.HIGHEST, preferred_element_type=F32
            )
        gram[x] = jnp.concatenate([total, jnp.zeros((pair, LANES - pair), F32)], axis=1)
        for d in range(1, m):
            gram_copies.append(
                send(gram.at[x], gram.at[x], mod_s.at[0, d - 1], mod_r.at[0, d - 1], other(d))
            )

    inverses = []

    def solve():
        for h in range(2):
            for l, value in enumerate(lefts(h)):
                high, low = split(value)
                stack[l, :, h * half : (h + 1) * half] = jnp.concatenate(
                    [high, high, low, low], axis=0
                )
        for copy in gram_copies:
            copy.wait_recv()
        total = gram[0]
        for i in range(1, m):
            total = total + gram[i]
        for l in range(layers):
            a = total[l * rank : (l + 1) * rank, :]
            sub = lax.broadcasted_iota(jnp.int32, a.shape, 0)
            lane = lax.broadcasted_iota(jnp.int32, a.shape, 1)
            diagonal = lane == sub + l * rank
            ridge = 0.001 * jnp.sum(jnp.where(diagonal, a, 0.0)) / rank
            a = a + jnp.where(diagonal, ridge, 0.0)
            a = invert(a, rank, l * rank)
            inside = (lane >= l * rank) & (lane < (l + 1) * rank)
            inverses.append(jnp.where(inside, a, 0.0)[:, :pair])

    total = reduce_scatter(r_part, r_core, r_sum, r_arrived, 1, make_gram, solve)
    waits.extend(gram_copies)
    r_model[x] = total
    swaps = [
        send(r_model.at[x], r_model.at[x], mod_s.at[1, d - 1], mod_r.at[1, d - 1], other(d))
        for d in range(1, m)
    ]
    for copy in swaps:
        copy.wait_recv()
    waits.extend(swaps)
    total = r_model[0]
    for i in range(1, m):
        total = total + r_model[i]
    right[pl.ds(pl.multiple_of((c * q + k) * rank, rank), rank), :] = total
    copies, forwards = gather_start(right, 1)

    mixed = jnp.dot(
        jnp.concatenate(inverses, axis=0),
        jnp.concatenate([total] * layers, axis=0),
        precision=lax.Precision.HIGHEST,
        preferred_element_type=F32,
    ) / n
    load_m.wait()
    load_w.wait()
    stores = []
    for l in range(layers):
        high, low = split(mixed[l * rank : (l + 1) * rank, l * wc : (l + 1) * wc])
        change = lax.dot_general(
            jnp.concatenate([high, low, high, low], axis=0), stack[l],
            (((0,), (0,)), ((), ())), preferred_element_type=F32,
        )
        new_m = 0.9 * mom[l] + change
        mom[l] = new_m
        w[l] = w[l] - 0.02 * new_m
        for src, dst, i in ((mom, out_m, 0), (w, out_w, 1)):
            copy = pltpu.make_async_copy(src.at[l], dst.at[l], load_sem.at[3 + 2 * l + i])
            copy.start()
            stores.append(copy)

    gather_pass(right, 1, copies, forwards)
    gather_end(copies, forwards)
    squares = jnp.zeros((rank, LANES), F32)
    for pos in range(n):
        value = right[pos * rank : (pos + 1) * rank, :]
        squares = squares + value * value
    lane = lax.broadcasted_iota(jnp.int32, squares.shape, 1)
    scales = [
        lax.rsqrt(
            jnp.sum(
                jnp.where((lane >= l * wc) & (lane < (l + 1) * wc), squares, 0.0),
                axis=(0, 1), keepdims=True,
            ) / (width * rank) + 1e-12
        )
        for l in range(layers)
    ]
    for idx in range(n):
        at = ((idx % 2) * q + idx // 2) * rank
        value = right[at : at + rank, :]
        for l in range(layers):
            basis_out[l, :, idx * wc : (idx + 1) * wc] = value[:, l * wc : (l + 1) * wc] * scales[l]
    copy = pltpu.make_async_copy(basis_out, out_b, load_sem.at[0])
    copy.start()
    stores.append(copy)
    for copy in waits:
        copy.wait_send()
    for copy in stores:
        copy.wait()


def write_out(*refs):
    sems = refs[-1]
    copies = [
        pltpu.make_async_copy(refs[i], refs[i + 3], sems.at[i]) for i in range(3)
    ]
    for copy in copies:
        copy.start()
    for copy in copies:
        copy.wait()


def shards(n, m, layer_grads, last_basis, layer_weights, momentum):
    _, layers, rows, width = layer_grads.shape
    last_basis, layer_weights, momentum = (
        jnp.swapaxes(a, 1, 2) for a in (last_basis, layer_weights, momentum)
    )
    rank = last_basis.shape[1]
    pair = layers * rank
    q = n // 2
    tall = rows // LANES * pair
    dma = pltpu.SemaphoreType.DMA
    vmem = pltpu.VMEM
    outs = pl.pallas_call(
        functools.partial(kernel, n, m),
        out_shape=(
            jax.ShapeDtypeStruct(layer_weights.shape, F32),
            jax.ShapeDtypeStruct(last_basis.shape, F32),
            jax.ShapeDtypeStruct(momentum.shape, F32),
        ),
        in_specs=[pl.BlockSpec(memory_space=pltpu.HBM)] * 4,
        out_specs=[pl.BlockSpec(memory_space=pl.ANY)] * 3,
        scratch_shapes=[
            vmem((layers, rows, width), BF16),
            vmem(last_basis.shape, F32),
            vmem(layer_weights.shape, F32),
            vmem(momentum.shape, F32),
            vmem((layers, 4 * rank, rows), BF16),
            vmem((tall, LANES), F32),
            vmem((tall // 2, LANES), F32),
            vmem((tall // 2, LANES), F32),
            vmem((q - 1, tall // n, LANES), F32),
            vmem((tall, LANES), F32),
            vmem((n * rank, LANES), F32),
            vmem((q * rank, LANES), F32),
            vmem((q * rank, LANES), F32),
            vmem((q - 1, rank, LANES), F32),
            vmem((m, rank, LANES), F32),
            vmem((n * rank, LANES), F32),
            vmem((m, pair, LANES), F32),
            vmem(last_basis.shape, F32),
            dma((3 + 2 * layers,)),
            dma((2,)), dma((2,)),
            dma((2, q - 1)), dma((2, q - 1)),
            dma((2, q - 1)), dma((2, q - 1)),
            dma((2, q)), dma((2, q)),
            dma((2, m - 1)), dma((2, m - 1)),
        ],
        compiler_params=pltpu.CompilerParams(
            collective_id=0, has_side_effects=True, vmem_limit_bytes=LIMIT
        ),
        name="step",
    )(
        *(
            pltpu.with_memory_space_constraint(a, pltpu.HBM)
            for a in (layer_grads, last_basis, layer_weights, momentum)
        )
    )
    outs = pl.pallas_call(
        write_out,
        out_shape=tuple(jax.ShapeDtypeStruct(a.shape, F32) for a in outs),
        in_specs=[pl.BlockSpec(memory_space=pl.ANY)] * 3,
        out_specs=[pl.BlockSpec(memory_space=pltpu.HBM)] * 3,
        scratch_shapes=[dma((3,))],
        compiler_params=pltpu.CompilerParams(vmem_limit_bytes=LIMIT2),
        name="write_out",
    )(*outs)
    return tuple(jnp.swapaxes(a, 1, 2) for a in outs)


def solution(mesh):
    in_specs = (
        P("replica", None, "model", None),
        P(),
        P(None, "model", "replica"),
        P(None, "model", "replica"),
    )
    out_specs = (P(None, "model", "replica"), P(), P(None, "model", "replica"))
    body = functools.partial(shards, mesh.shape["replica"], mesh.shape["model"])
    return jax.shard_map(body, mesh=mesh, in_specs=in_specs, out_specs=out_specs, check_vma=False)
```

```python
import functools

import jax
import jax.numpy as jnp
from jax import lax
from jax.experimental import pallas as pl
from jax.experimental.pallas import tpu as pltpu
from jax.sharding import PartitionSpec as P

LANES = 128
MIB = 1024 * 1024
LIMIT = 32 * MIB
LIMIT2 = 16 * MIB
F32 = jnp.float32
BF16 = jnp.bfloat16
NT = (((1,), (1,)), ((), ()))


def split(value):
    high = value.astype(BF16)
    return high, (value - high.astype(F32)).astype(BF16)


def invert(a, rank, first):
    lane = lax.broadcasted_iota(jnp.int32, a.shape, 1)
    sub = lax.broadcasted_iota(jnp.int32, a.shape, 0)
    for p in range(rank):
        at = first + p
        row = a[p : p + 1, :]
        col = a[:, at : at + 1]
        inverse = 1.0 / a[p : p + 1, at : at + 1]
        row = jnp.where(lane[:1] == at, 1.0, row) * inverse
        a = jnp.where(sub == p, row, jnp.where(lane == at, 0.0, a) - col * row)
    return a


def kernel(
    n, m, grads, basis, weights, momentum, out_w, out_b, out_m,
    g, b, w, mom, stack, part, from_core, summed, arrived, left,
    r_part, r_core, r_sum, r_arrived, r_model, right, gram, basis_out,
    load_sem, core_s, core_r, rs_s, rs_r, ag_s, ag_r, fwd_s, fwd_r,
    mod_s, mod_r,
):
    layers, rows, width = g.shape
    rank = b.shape[1]
    pair = layers * rank
    groups = part.shape[0]
    deep = layers // groups
    q = n // 2
    half = rows // 2
    blocks = half // LANES
    wc = width // n
    me = lax.axis_index("replica")
    x = lax.axis_index("model")
    c, k = lax.rem(me, 2), me // 2
    o = 1 - c

    def near(d):
        return lax.rem(k + d, q)

    def before(d):
        return lax.rem(k + q - d, q)

    def send(src, dst, s, r, device):
        copy = pltpu.make_async_remote_copy(
            src_ref=src, dst_ref=dst, send_sem=s, recv_sem=r,
            device_id=device, device_id_type=pl.DeviceIdType.MESH,
        )
        copy.start()
        return copy

    partner = {"replica": 2 * k + o}

    def chip(d):
        return {"replica": 2 * near(d) + c}

    def other(d):
        return {"model": lax.rem(x + d, m)}

    def rows_of(h):
        return pl.ds(pl.multiple_of(h * half, half), half)

    load_b = pltpu.make_async_copy(basis, b, load_sem.at[0])
    load_b.start()
    loads = []
    for l in range(layers):
        for i, h in enumerate((o, c)):
            copy = pltpu.make_async_copy(
                grads.at[0, l, rows_of(h)], g.at[l, rows_of(h)], load_sem.at[3 + 2 * l + i]
            )
            copy.start()
            loads.append(copy)
    load_m = pltpu.make_async_copy(momentum, mom, load_sem.at[1])
    load_w = pltpu.make_async_copy(weights, w, load_sem.at[2])
    load_m.start()
    load_w.start()

    barrier = pltpu.get_barrier_semaphore()
    peers = [partner] + [chip(d) for d in range(1, q)] + [other(d) for d in range(1, m)]
    for device in peers:
        pl.semaphore_signal(
            barrier, inc=1, device_id=device, device_id_type=pl.DeviceIdType.MESH
        )

    load_b.wait()
    turned = [b[l].astype(BF16) for l in range(layers)]

    def block_of(h, j, l):
        at = ((h * blocks + j) * deep + l % deep) * rank
        return pl.ds(pl.multiple_of(at, rank), rank)

    def part_of(h, i, group):
        for l in range(group * deep, (group + 1) * deep):
            loads[2 * l + i].wait()
            value = lax.dot_general(
                turned[l], g[l, rows_of(h), :], NT, preferred_element_type=F32
            )
            for j in range(blocks):
                part[group, block_of(h, j, l), :] = value[:, j * LANES : (j + 1) * LANES]

    waits = []

    def halves(buf):
        size = buf.shape[0] // 2
        return [pl.ds(pl.multiple_of(h * size, size), size) for h in (c, o)]

    def core_start(source, near_buf, phase):
        theirs = halves(source)[1]
        copy = send(source.at[theirs], near_buf, core_s.at[phase], core_r.at[phase], partner)
        waits.append(copy)
        return copy

    def scatter_start(core, source, near_buf, sums, far_buf, phase):
        mine = halves(source)[0]
        share = sums.shape[0] // q
        core.wait_recv()
        sums[...] = source[mine, :] + near_buf[...]
        copies = []
        for d in range(1, q):
            to = pl.ds(pl.multiple_of(near(d) * share, share), share)
            copies.append(
                send(sums.at[to], far_buf.at[d - 1], rs_s.at[phase, d - 1],
                     rs_r.at[phase, d - 1], chip(d))
            )
        waits.extend(copies)
        return copies

    def scatter_end(copies, sums, far_buf):
        share = sums.shape[0] // q
        total = sums[pl.ds(pl.multiple_of(k * share, share), share), :]
        for d in range(1, q):
            copies[d - 1].wait_recv()
            total = total + far_buf[d - 1]
        return total

    def gather_start(buf, phase):
        share = buf.shape[0] // n
        own = pl.ds(pl.multiple_of((c * q + k) * share, share), share)
        copies = [
            send(buf.at[own], buf.at[own], ag_s.at[phase, d - 1], ag_r.at[phase, d - 1], chip(d))
            for d in range(1, q)
        ]
        forwards = [
            send(buf.at[own], buf.at[own], fwd_s.at[phase, 0], fwd_r.at[phase, 0], partner)
        ]
        return copies, forwards

    def gather_pass(buf, phase, copies, forwards):
        share = buf.shape[0] // n
        for d in range(1, q):
            copies[d - 1].wait_recv()
            at = pl.ds(pl.multiple_of((c * q + before(d)) * share, share), share)
            forwards.append(
                send(buf.at[at], buf.at[at], fwd_s.at[phase, d], fwd_r.at[phase, d], partner)
            )

    def gather_end(copies, forwards):
        for copy in forwards:
            copy.wait_recv()
        waits.extend(copies + forwards)

    scatters = []
    for group in range(groups):
        part_of(o, 0, group)
        if group == 0:
            pl.semaphore_wait(barrier, len(peers))
        core = core_start(part.at[group], from_core.at[group], group)
        part_of(c, 1, group)
        scatters.append(
            scatter_start(core, part.at[group], from_core.at[group], summed.at[group],
                          arrived.at[group], group)
        )
    gathers = []
    size = part.shape[1] // n
    for group in range(groups):
        share = scatter_end(scatters[group], summed.at[group], arrived.at[group])
        left[group, pl.ds(pl.multiple_of((c * q + k) * size, size), size), :] = share
        gathers.append(gather_start(left.at[group], group))

    def left_of(h, l):
        return jnp.concatenate(
            [left[l // deep, block_of(h, j, l), :] for j in range(blocks)], axis=1
        )

    def lefts(h):
        return [left_of(h, l) for l in range(layers)]

    def right_of(h, l):
        return jnp.dot(
            left_of(h, l).astype(BF16), g[l, rows_of(h), :], preferred_element_type=F32
        )

    own_right = []
    for group in range(groups):
        gather_pass(left.at[group], group, *gathers[group])
        members = range(group * deep, (group + 1) * deep)
        firsts = [right_of(c, l) for l in members]
        gather_end(*gathers[group])
        own_right.extend(a + right_of(o, l) for a, l in zip(firsts, members))
    if layers * wc < LANES:
        r_part[...] = jnp.zeros_like(r_part)
    for idx in range(n):
        at = ((idx % 2) * q + idx // 2) * rank
        for l in range(layers):
            r_part[at : at + rank, l * wc : (l + 1) * wc] = own_right[l][:, idx * wc : (idx + 1) * wc]

    gram_copies = []

    def make_gram():
        total = jnp.zeros((pair, pair), F32)
        for h in range(2):
            both = jnp.concatenate(lefts(h), axis=0)
            total = total + lax.dot_general(
                both, both, NT, precision=lax.Precision.HIGHEST, preferred_element_type=F32
            )
        gram[x] = jnp.concatenate([total, jnp.zeros((pair, LANES - pair), F32)], axis=1)
        for d in range(1, m):
            gram_copies.append(
                send(gram.at[x], gram.at[x], mod_s.at[0, d - 1], mod_r.at[0, d - 1], other(d))
            )

    inverses = []

    def solve():
        for h in range(2):
            for l, value in enumerate(lefts(h)):
                high, low = split(value)
                stack[l, :, h * half : (h + 1) * half] = jnp.concatenate(
                    [high, high, low, low], axis=0
                )
        for copy in gram_copies:
            copy.wait_recv()
        total = gram[0]
        for i in range(1, m):
            total = total + gram[i]
        for l in range(layers):
            a = total[l * rank : (l + 1) * rank, :]
            sub = lax.broadcasted_iota(jnp.int32, a.shape, 0)
            lane = lax.broadcasted_iota(jnp.int32, a.shape, 1)
            diagonal = lane == sub + l * rank
            ridge = 0.001 * jnp.sum(jnp.where(diagonal, a, 0.0)) / rank
            a = a + jnp.where(diagonal, ridge, 0.0)
            a = invert(a, rank, l * rank)
            inside = (lane >= l * rank) & (lane < (l + 1) * rank)
            inverses.append(jnp.where(inside, a, 0.0)[:, :pair])

    core = core_start(r_part, r_core, groups)
    make_gram()
    copies = scatter_start(core, r_part, r_core, r_sum, r_arrived, groups)
    solve()
    total = scatter_end(copies, r_sum, r_arrived)
    waits.extend(gram_copies)
    r_model[x] = total
    swaps = [
        send(r_model.at[x], r_model.at[x], mod_s.at[1, d - 1], mod_r.at[1, d - 1], other(d))
        for d in range(1, m)
    ]
    for copy in swaps:
        copy.wait_recv()
    waits.extend(swaps)
    total = r_model[0]
    for i in range(1, m):
        total = total + r_model[i]
    right[pl.ds(pl.multiple_of((c * q + k) * rank, rank), rank), :] = total
    copies, forwards = gather_start(right, groups)

    mixed = jnp.dot(
        jnp.concatenate(inverses, axis=0),
        jnp.concatenate([total] * layers, axis=0),
        precision=lax.Precision.HIGHEST,
        preferred_element_type=F32,
    ) / n
    load_m.wait()
    load_w.wait()
    stores = []
    for l in range(layers):
        high, low = split(mixed[l * rank : (l + 1) * rank, l * wc : (l + 1) * wc])
        change = lax.dot_general(
            jnp.concatenate([high, low, high, low], axis=0), stack[l],
            (((0,), (0,)), ((), ())), preferred_element_type=F32,
        )
        new_m = 0.9 * mom[l] + change
        mom[l] = new_m
        w[l] = w[l] - 0.02 * new_m
        for src, dst, i in ((mom, out_m, 0), (w, out_w, 1)):
            copy = pltpu.make_async_copy(src.at[l], dst.at[l], load_sem.at[3 + 2 * l + i])
            copy.start()
            stores.append(copy)

    gather_pass(right, groups, copies, forwards)
    gather_end(copies, forwards)
    squares = jnp.zeros((rank, LANES), F32)
    for pos in range(n):
        value = right[pos * rank : (pos + 1) * rank, :]
        squares = squares + value * value
    lane = lax.broadcasted_iota(jnp.int32, squares.shape, 1)
    scales = [
        lax.rsqrt(
            jnp.sum(
                jnp.where((lane >= l * wc) & (lane < (l + 1) * wc), squares, 0.0),
                axis=(0, 1), keepdims=True,
            ) / (width * rank) + 1e-12
        )
        for l in range(layers)
    ]
    for idx in range(n):
        at = ((idx % 2) * q + idx // 2) * rank
        value = right[at : at + rank, :]
        for l in range(layers):
            basis_out[l, :, idx * wc : (idx + 1) * wc] = value[:, l * wc : (l + 1) * wc] * scales[l]
    copy = pltpu.make_async_copy(basis_out, out_b, load_sem.at[0])
    copy.start()
    stores.append(copy)
    for copy in waits:
        copy.wait_send()
    for copy in stores:
        copy.wait()


def write_out(*refs):
    sems = refs[-1]
    copies = [
        pltpu.make_async_copy(refs[i], refs[i + 3], sems.at[i]) for i in range(3)
    ]
    for copy in copies:
        copy.start()
    for copy in copies:
        copy.wait()


def shards(n, m, layer_grads, last_basis, layer_weights, momentum):
    _, layers, rows, width = layer_grads.shape
    last_basis, layer_weights, momentum = (
        jnp.swapaxes(a, 1, 2) for a in (last_basis, layer_weights, momentum)
    )
    rank = last_basis.shape[1]
    pair = layers * rank
    q = n // 2
    tall = rows // LANES * pair
    groups = layers if tall // layers % (8 * n) == 0 else 1
    deep = tall // groups
    dma = pltpu.SemaphoreType.DMA
    vmem = pltpu.VMEM
    outs = pl.pallas_call(
        functools.partial(kernel, n, m),
        out_shape=(
            jax.ShapeDtypeStruct(layer_weights.shape, F32),
            jax.ShapeDtypeStruct(last_basis.shape, F32),
            jax.ShapeDtypeStruct(momentum.shape, F32),
        ),
        in_specs=[pl.BlockSpec(memory_space=pltpu.HBM)] * 4,
        out_specs=[pl.BlockSpec(memory_space=pl.ANY)] * 3,
        scratch_shapes=[
            vmem((layers, rows, width), BF16),
            vmem(last_basis.shape, F32),
            vmem(layer_weights.shape, F32),
            vmem(momentum.shape, F32),
            vmem((layers, 4 * rank, rows), BF16),
            vmem((groups, deep, LANES), F32),
            vmem((groups, deep // 2, LANES), F32),
            vmem((groups, deep // 2, LANES), F32),
            vmem((groups, q - 1, deep // n, LANES), F32),
            vmem((groups, deep, LANES), F32),
            vmem((n * rank, LANES), F32),
            vmem((q * rank, LANES), F32),
            vmem((q * rank, LANES), F32),
            vmem((q - 1, rank, LANES), F32),
            vmem((m, rank, LANES), F32),
            vmem((n * rank, LANES), F32),
            vmem((m, pair, LANES), F32),
            vmem(last_basis.shape, F32),
            dma((3 + 2 * layers,)),
            dma((groups + 1,)), dma((groups + 1,)),
            dma((groups + 1, q - 1)), dma((groups + 1, q - 1)),
            dma((groups + 1, q - 1)), dma((groups + 1, q - 1)),
            dma((groups + 1, q)), dma((groups + 1, q)),
            dma((2, m - 1)), dma((2, m - 1)),
        ],
        compiler_params=pltpu.CompilerParams(
            collective_id=0, has_side_effects=True, vmem_limit_bytes=LIMIT
        ),
        name="step",
    )(
        *(
            pltpu.with_memory_space_constraint(a, pltpu.HBM)
            for a in (layer_grads, last_basis, layer_weights, momentum)
        )
    )
    outs = pl.pallas_call(
        write_out,
        out_shape=tuple(jax.ShapeDtypeStruct(a.shape, F32) for a in outs),
        in_specs=[pl.BlockSpec(memory_space=pl.ANY)] * 3,
        out_specs=[pl.BlockSpec(memory_space=pltpu.HBM)] * 3,
        scratch_shapes=[dma((3,))],
        compiler_params=pltpu.CompilerParams(vmem_limit_bytes=LIMIT2),
        name="write_out",
    )(*outs)
    return tuple(jnp.swapaxes(a, 1, 2) for a in outs)


def solution(mesh):
    in_specs = (
        P("replica", None, "model", None),
        P(),
        P(None, "model", "replica"),
        P(None, "model", "replica"),
    )
    out_specs = (P(None, "model", "replica"), P(), P(None, "model", "replica"))
    body = functools.partial(shards, mesh.shape["replica"], mesh.shape["model"])
    return jax.shard_map(body, mesh=mesh, in_specs=in_specs, out_specs=out_specs, check_vma=False)
```

```python
import functools

import jax
import jax.numpy as jnp
from jax import lax
from jax.experimental import pallas as pl
from jax.experimental.pallas import tpu as pltpu
from jax.sharding import PartitionSpec as P

LANES = 128
MIB = 1024 * 1024
LIMIT = 32 * MIB
LIMIT2 = 16 * MIB
F32 = jnp.float32
BF16 = jnp.bfloat16
NT = (((1,), (1,)), ((), ()))


def split(value):
    high = value.astype(BF16)
    return high, (value - high.astype(F32)).astype(BF16)


def invert(a, rank, first):
    lane = lax.broadcasted_iota(jnp.int32, a.shape, 1)
    sub = lax.broadcasted_iota(jnp.int32, a.shape, 0)
    for p in range(rank):
        at = first + p
        row = a[p : p + 1, :]
        col = a[:, at : at + 1]
        inverse = 1.0 / a[p : p + 1, at : at + 1]
        row = jnp.where(lane[:1] == at, 1.0, row) * inverse
        a = jnp.where(sub == p, row, jnp.where(lane == at, 0.0, a) - col * row)
    return a


def kernel(
    n, m, grads, basis, weights, momentum, out_w, out_b, out_m,
    g, b, w, mom, stack, part, from_core, summed, arrived, left,
    r_part, r_core, r_sum, r_arrived, r_model, right, gram, basis_out,
    load_sem, core_s, core_r, rs_s, rs_r, ag_s, ag_r, fwd_s, fwd_r,
    mod_s, mod_r,
):
    layers, rows, width = g.shape
    rank = b.shape[1]
    pair = layers * rank
    groups = part.shape[0]
    deep = layers // groups
    q = n // 2
    half = rows // 2
    blocks = half // LANES
    wc = width // n
    me = lax.axis_index("replica")
    x = lax.axis_index("model")
    c, k = lax.rem(me, 2), me // 2
    o = 1 - c

    def near(d):
        return lax.rem(k + d, q)

    def before(d):
        return lax.rem(k + q - d, q)

    def send(src, dst, s, r, device):
        copy = pltpu.make_async_remote_copy(
            src_ref=src, dst_ref=dst, send_sem=s, recv_sem=r,
            device_id=device, device_id_type=pl.DeviceIdType.MESH,
        )
        copy.start()
        return copy

    partner = {"replica": 2 * k + o}

    def chip(d):
        return {"replica": 2 * near(d) + c}

    wide = max(e for e in range(1, q + 1) if q % e == 0 and e * e <= q)
    far = q // wide
    row, col = k // wide, lax.rem(k, wide)

    def cell(a, e):
        at = lax.rem(row + a, far) * wide + lax.rem(col + e, wide)
        return {"replica": 2 * at + c}

    def other(d):
        return {"model": lax.rem(x + d, m)}

    def rows_of(h):
        return pl.ds(pl.multiple_of(h * half, half), half)

    load_b = pltpu.make_async_copy(basis, b, load_sem.at[0])
    load_b.start()
    loads = []
    for l in range(layers):
        for i, h in enumerate((o, c)):
            copy = pltpu.make_async_copy(
                grads.at[0, l, rows_of(h)], g.at[l, rows_of(h)], load_sem.at[3 + 2 * l + i]
            )
            copy.start()
            loads.append(copy)
    load_m = pltpu.make_async_copy(momentum, mom, load_sem.at[1])
    load_w = pltpu.make_async_copy(weights, w, load_sem.at[2])
    load_m.start()
    load_w.start()

    barrier = pltpu.get_barrier_semaphore()
    peers = [partner] + [chip(d) for d in range(1, q)] + [other(d) for d in range(1, m)]
    for device in peers:
        pl.semaphore_signal(
            barrier, inc=1, device_id=device, device_id_type=pl.DeviceIdType.MESH
        )

    load_b.wait()
    turned = [b[l].astype(BF16) for l in range(layers)]

    def block_of(h, j, l):
        at = ((h * blocks + j) * deep + l % deep) * rank
        return pl.ds(pl.multiple_of(at, rank), rank)

    def part_of(h, i, group):
        for l in range(group * deep, (group + 1) * deep):
            loads[2 * l + i].wait()
            value = lax.dot_general(
                turned[l], g[l, rows_of(h), :], NT, preferred_element_type=F32
            )
            for j in range(blocks):
                part[group, block_of(h, j, l), :] = value[:, j * LANES : (j + 1) * LANES]

    waits = []

    def halves(buf):
        size = buf.shape[0] // 2
        return [pl.ds(pl.multiple_of(h * size, size), size) for h in (c, o)]

    def core_start(source, near_buf, phase):
        theirs = halves(source)[1]
        copy = send(source.at[theirs], near_buf, core_s.at[phase], core_r.at[phase], partner)
        waits.append(copy)
        return copy

    def scatter_start(core, source, near_buf, sums, far_buf, phase):
        mine = halves(source)[0]
        share = sums.shape[0] // q
        core.wait_recv()
        sums[...] = source[mine, :] + near_buf[...]
        copies = []
        for d in range(1, q):
            to = pl.ds(pl.multiple_of(near(d) * share, share), share)
            copies.append(
                send(sums.at[to], far_buf.at[d - 1], rs_s.at[phase, d - 1],
                     rs_r.at[phase, d - 1], chip(d))
            )
        waits.extend(copies)
        return copies

    def scatter_end(copies, sums, far_buf):
        share = sums.shape[0] // q
        total = sums[pl.ds(pl.multiple_of(k * share, share), share), :]
        for d in range(1, q):
            copies[d - 1].wait_recv()
            total = total + far_buf[d - 1]
        return total

    def gather_start(buf, phase):
        share = buf.shape[0] // n
        own = pl.ds(pl.multiple_of((c * q + k) * share, share), share)
        copies = [
            send(buf.at[own], buf.at[own], ag_s.at[phase, d - 1], ag_r.at[phase, d - 1], chip(d))
            for d in range(1, q)
        ]
        forwards = [
            send(buf.at[own], buf.at[own], fwd_s.at[phase, 0], fwd_r.at[phase, 0], partner)
        ]
        return copies, forwards

    def gather_pass(buf, phase, copies, forwards):
        share = buf.shape[0] // n
        for d in range(1, q):
            copies[d - 1].wait_recv()
            at = pl.ds(pl.multiple_of((c * q + before(d)) * share, share), share)
            forwards.append(
                send(buf.at[at], buf.at[at], fwd_s.at[phase, d], fwd_r.at[phase, d], partner)
            )

    def spread_start(buf, phase):
        share = buf.shape[0] // n
        own = pl.ds(pl.multiple_of((c * q + k) * share, share), share)
        copies = {}
        for a, e in [(a, 0) for a in range(1, far)] + [(0, e) for e in range(1, wide)]:
            copies[a, e] = send(
                buf.at[own], buf.at[own], ag_s.at[phase, a * wide + e - 1],
                ag_r.at[phase, a * wide + e - 1], cell(a, e),
            )
        forwards = [
            send(buf.at[own], buf.at[own], fwd_s.at[phase, 0], fwd_r.at[phase, 0], partner)
        ]
        return copies, forwards

    def spread_pass(buf, phase, copies, forwards):
        share = buf.shape[0] // n
        order = [(a, 0) for a in range(1, far)]
        order += [(a, e) for a in range(far) for e in range(1, wide)]
        for a, e in order:
            copies[a, e].wait_recv()
            at = (c * q + lax.rem(row + far - a, far) * wide + lax.rem(col + wide - e, wide)) * share
            at = pl.ds(pl.multiple_of(at, share), share)
            if e == 0:
                for f in range(1, wide):
                    copies[a, f] = send(
                        buf.at[at], buf.at[at], ag_s.at[phase, a * wide + f - 1],
                        ag_r.at[phase, a * wide + f - 1], cell(0, f),
                    )
            forwards.append(
                send(buf.at[at], buf.at[at], fwd_s.at[phase, a * wide + e],
                     fwd_r.at[phase, a * wide + e], partner)
            )

    def gather_end(copies, forwards):
        for copy in forwards:
            copy.wait_recv()
        waits.extend(list(copies.values()) if isinstance(copies, dict) else copies)
        waits.extend(forwards)

    scatters = []
    for group in range(groups):
        part_of(o, 0, group)
        if group == 0:
            pl.semaphore_wait(barrier, len(peers))
        core = core_start(part.at[group], from_core.at[group], group)
        part_of(c, 1, group)
        scatters.append(
            scatter_start(core, part.at[group], from_core.at[group], summed.at[group],
                          arrived.at[group], group)
        )
    gathers = []
    size = part.shape[1] // n
    for group in range(groups):
        share = scatter_end(scatters[group], summed.at[group], arrived.at[group])
        left[group, pl.ds(pl.multiple_of((c * q + k) * size, size), size), :] = share
        gathers.append(spread_start(left.at[group], group))

    def left_of(h, l):
        return jnp.concatenate(
            [left[l // deep, block_of(h, j, l), :] for j in range(blocks)], axis=1
        )

    def lefts(h):
        return [left_of(h, l) for l in range(layers)]

    def right_of(h, l):
        return jnp.dot(
            left_of(h, l).astype(BF16), g[l, rows_of(h), :], preferred_element_type=F32
        )

    own_right = []
    for group in range(groups):
        spread_pass(left.at[group], group, *gathers[group])
        members = range(group * deep, (group + 1) * deep)
        firsts = [right_of(c, l) for l in members]
        gather_end(*gathers[group])
        own_right.extend(a + right_of(o, l) for a, l in zip(firsts, members))
    if layers * wc < LANES:
        r_part[...] = jnp.zeros_like(r_part)
    for idx in range(n):
        at = ((idx % 2) * q + idx // 2) * rank
        for l in range(layers):
            r_part[at : at + rank, l * wc : (l + 1) * wc] = own_right[l][:, idx * wc : (idx + 1) * wc]

    gram_copies = []

    def make_gram():
        total = jnp.zeros((pair, pair), F32)
        for h in range(2):
            both = jnp.concatenate(lefts(h), axis=0)
            total = total + lax.dot_general(
                both, both, NT, precision=lax.Precision.HIGHEST, preferred_element_type=F32
            )
        gram[x] = jnp.concatenate([total, jnp.zeros((pair, LANES - pair), F32)], axis=1)
        for d in range(1, m):
            gram_copies.append(
                send(gram.at[x], gram.at[x], mod_s.at[0, d - 1], mod_r.at[0, d - 1], other(d))
            )

    inverses = []

    def solve():
        for h in range(2):
            for l, value in enumerate(lefts(h)):
                high, low = split(value)
                stack[l, :, h * half : (h + 1) * half] = jnp.concatenate(
                    [high, high, low, low], axis=0
                )
        for copy in gram_copies:
            copy.wait_recv()
        total = gram[0]
        for i in range(1, m):
            total = total + gram[i]
        for l in range(layers):
            a = total[l * rank : (l + 1) * rank, :]
            sub = lax.broadcasted_iota(jnp.int32, a.shape, 0)
            lane = lax.broadcasted_iota(jnp.int32, a.shape, 1)
            diagonal = lane == sub + l * rank
            ridge = 0.001 * jnp.sum(jnp.where(diagonal, a, 0.0)) / rank
            a = a + jnp.where(diagonal, ridge, 0.0)
            a = invert(a, rank, l * rank)
            inside = (lane >= l * rank) & (lane < (l + 1) * rank)
            inverses.append(jnp.where(inside, a, 0.0)[:, :pair])

    core = core_start(r_part, r_core, groups)
    make_gram()
    copies = scatter_start(core, r_part, r_core, r_sum, r_arrived, groups)
    solve()
    total = scatter_end(copies, r_sum, r_arrived)
    waits.extend(gram_copies)
    r_model[x] = total
    swaps = [
        send(r_model.at[x], r_model.at[x], mod_s.at[1, d - 1], mod_r.at[1, d - 1], other(d))
        for d in range(1, m)
    ]
    for copy in swaps:
        copy.wait_recv()
    waits.extend(swaps)
    total = r_model[0]
    for i in range(1, m):
        total = total + r_model[i]
    right[pl.ds(pl.multiple_of((c * q + k) * rank, rank), rank), :] = total
    copies, forwards = gather_start(right, groups)

    mixed = jnp.dot(
        jnp.concatenate(inverses, axis=0),
        jnp.concatenate([total] * layers, axis=0),
        precision=lax.Precision.HIGHEST,
        preferred_element_type=F32,
    ) / n
    load_m.wait()
    load_w.wait()
    stores = []
    for l in range(layers):
        high, low = split(mixed[l * rank : (l + 1) * rank, l * wc : (l + 1) * wc])
        change = lax.dot_general(
            jnp.concatenate([high, low, high, low], axis=0), stack[l],
            (((0,), (0,)), ((), ())), preferred_element_type=F32,
        )
        new_m = 0.9 * mom[l] + change
        mom[l] = new_m
        w[l] = w[l] - 0.02 * new_m
        for src, dst, i in ((mom, out_m, 0), (w, out_w, 1)):
            copy = pltpu.make_async_copy(src.at[l], dst.at[l], load_sem.at[3 + 2 * l + i])
            copy.start()
            stores.append(copy)

    gather_pass(right, groups, copies, forwards)
    gather_end(copies, forwards)
    squares = jnp.zeros((rank, LANES), F32)
    for pos in range(n):
        value = right[pos * rank : (pos + 1) * rank, :]
        squares = squares + value * value
    lane = lax.broadcasted_iota(jnp.int32, squares.shape, 1)
    scales = [
        lax.rsqrt(
            jnp.sum(
                jnp.where((lane >= l * wc) & (lane < (l + 1) * wc), squares, 0.0),
                axis=(0, 1), keepdims=True,
            ) / (width * rank) + 1e-12
        )
        for l in range(layers)
    ]
    for idx in range(n):
        at = ((idx % 2) * q + idx // 2) * rank
        value = right[at : at + rank, :]
        for l in range(layers):
            basis_out[l, :, idx * wc : (idx + 1) * wc] = value[:, l * wc : (l + 1) * wc] * scales[l]
    copy = pltpu.make_async_copy(basis_out, out_b, load_sem.at[0])
    copy.start()
    stores.append(copy)
    for copy in waits:
        copy.wait_send()
    for copy in stores:
        copy.wait()


def write_out(*refs):
    sems = refs[-1]
    copies = [
        pltpu.make_async_copy(refs[i], refs[i + 3], sems.at[i]) for i in range(3)
    ]
    for copy in copies:
        copy.start()
    for copy in copies:
        copy.wait()


def shards(n, m, layer_grads, last_basis, layer_weights, momentum):
    _, layers, rows, width = layer_grads.shape
    last_basis, layer_weights, momentum = (
        jnp.swapaxes(a, 1, 2) for a in (last_basis, layer_weights, momentum)
    )
    rank = last_basis.shape[1]
    pair = layers * rank
    q = n // 2
    tall = rows // LANES * pair
    groups = layers if tall // layers % (8 * n) == 0 else 1
    deep = tall // groups
    dma = pltpu.SemaphoreType.DMA
    vmem = pltpu.VMEM
    outs = pl.pallas_call(
        functools.partial(kernel, n, m),
        out_shape=(
            jax.ShapeDtypeStruct(layer_weights.shape, F32),
            jax.ShapeDtypeStruct(last_basis.shape, F32),
            jax.ShapeDtypeStruct(momentum.shape, F32),
        ),
        in_specs=[pl.BlockSpec(memory_space=pltpu.HBM)] * 4,
        out_specs=[pl.BlockSpec(memory_space=pl.ANY)] * 3,
        scratch_shapes=[
            vmem((layers, rows, width), BF16),
            vmem(last_basis.shape, F32),
            vmem(layer_weights.shape, F32),
            vmem(momentum.shape, F32),
            vmem((layers, 4 * rank, rows), BF16),
            vmem((groups, deep, LANES), F32),
            vmem((groups, deep // 2, LANES), F32),
            vmem((groups, deep // 2, LANES), F32),
            vmem((groups, q - 1, deep // n, LANES), F32),
            vmem((groups, deep, LANES), F32),
            vmem((n * rank, LANES), F32),
            vmem((q * rank, LANES), F32),
            vmem((q * rank, LANES), F32),
            vmem((q - 1, rank, LANES), F32),
            vmem((m, rank, LANES), F32),
            vmem((n * rank, LANES), F32),
            vmem((m, pair, LANES), F32),
            vmem(last_basis.shape, F32),
            dma((3 + 2 * layers,)),
            dma((groups + 1,)), dma((groups + 1,)),
            dma((groups + 1, q - 1)), dma((groups + 1, q - 1)),
            dma((groups + 1, q - 1)), dma((groups + 1, q - 1)),
            dma((groups + 1, q)), dma((groups + 1, q)),
            dma((2, m - 1)), dma((2, m - 1)),
        ],
        compiler_params=pltpu.CompilerParams(
            collective_id=0, has_side_effects=True, vmem_limit_bytes=LIMIT
        ),
        name="step",
    )(
        *(
            pltpu.with_memory_space_constraint(a, pltpu.HBM)
            for a in (layer_grads, last_basis, layer_weights, momentum)
        )
    )
    outs = pl.pallas_call(
        write_out,
        out_shape=tuple(jax.ShapeDtypeStruct(a.shape, F32) for a in outs),
        in_specs=[pl.BlockSpec(memory_space=pl.ANY)] * 3,
        out_specs=[pl.BlockSpec(memory_space=pltpu.HBM)] * 3,
        scratch_shapes=[dma((3,))],
        compiler_params=pltpu.CompilerParams(vmem_limit_bytes=LIMIT2),
        name="write_out",
    )(*outs)
    return tuple(jnp.swapaxes(a, 1, 2) for a in outs)


def solution(mesh):
    in_specs = (
        P("replica", None, "model", None),
        P(),
        P(None, "model", "replica"),
        P(None, "model", "replica"),
    )
    out_specs = (P(None, "model", "replica"), P(), P(None, "model", "replica"))
    body = functools.partial(shards, mesh.shape["replica"], mesh.shape["model"])
    return jax.shard_map(body, mesh=mesh, in_specs=in_specs, out_specs=out_specs, check_vma=False)
```
